32 devices in a mesh: owner: 4 (over y, core), rows: 8 (over z, x).
Axes of the slice: x: 2, y: 2, z: 4, core: 2. Of those that a mesh axis runs over, the one named last changes fastest.
Arguments:
- train_gate: float32 [64, 2048, 1024], P('owner', 'rows'), may hold values from -0.1875 to 0.1875
- other_gate: bfloat16 [64, 2048, 1024], P('owner', 'rows'), may hold values from -0.0625 to 0.0625
- train_up: float32 [64, 2048, 1024], P('owner', 'rows'), may hold values from -0.1875 to 0.1875
- other_up: bfloat16 [64, 2048, 1024], P('owner', 'rows'), may hold values from -0.0625 to 0.0625
- train_down: float32 [64, 1024, 2048], P('owner', None, 'rows'), may hold values from -0.25 to 0.25
- other_down: bfloat16 [64, 1024, 2048], P('owner', None, 'rows'), may hold values from -0.09375 to 0.09375
- router_weight: float32 [2048, 64], P('rows', 'owner'), may hold values from -0.125 to 0.125
- router_gain: float32 [2048], P('rows'), may hold values from 0.25 to 1.75
Outputs:
- ready_gate: bfloat16 [64, 2048, 1024], P('owner', None, 'rows')
- ready_up: bfloat16 [64, 2048, 1024], P('owner', None, 'rows')
- ready_down: bfloat16 [64, 1024, 2048], P('owner', 'rows')
- scale_gate: float32 [64, 1024], P('owner', 'rows')
- scale_up: float32 [64, 1024], P('owner', 'rows')
- scale_down: float32 [64, 1024], P('owner', 'rows')
- serve_router: bfloat16 [2048, 64], replicated
The draws below stay inside these ranges and needn't reach their ends.
All inputs are finite; a program needn't handle non-finite values. Where the reference program divides by a largest or mean magnitude, that divisor is 1e-20 or more.
Results may differ from the reference program's by a relative error of at most 0.001.
Values may be sent and summed in bfloat16 or wider, within the bound.
A program may use at most 192 MiB of HBM per device.

```python
import jax
import jax.numpy as jnp

EXPERTS = 64
D_MODEL = 2048
D_EXPERT = 1024


def strengthened(values, own_key, source, target, parts, factor):
    def block_of(axis_at):
        return (jnp.arange(values.shape[axis_at]) // (values.shape[axis_at] // parts)).reshape((-1,) + (1,) * (values.ndim - 1 - axis_at))

    near = jax.random.permutation(own_key, parts)[block_of(target)]
    far = (block_of(target) + parts // 2) % parts
    return jnp.where((block_of(source) == near) | (block_of(source) == far), factor * values, values)


def shard_levels(key, shape, pieces, least, high):
    def one(dim, blocks):
        steps = jax.random.uniform(jax.random.fold_in(jax.random.fold_in(key, 6), dim), (blocks,), jnp.float32, least / len(pieces), high / len(pieces))
        return jnp.repeat(jnp.exp(steps), shape[dim] // blocks).reshape((-1,) + (1,) * (len(shape) - dim - 1))

    gain = one(*pieces[0])
    for cut in pieces[1:]:
        gain = gain * one(*cut)
    return gain


def bell_draw(own_key, shape, width, most, shards=(), held_as=jnp.bfloat16):
    values = jax.random.normal(own_key, shape, jnp.float32) * width
    if len(shards) > 0:
        values = shard_levels(own_key, shape, shards, -0.22, 0.18) * values
    return jnp.clip(values, min=-most, max=most).astype(held_as)


def gaussian_with(key, shape, deviation, limit, pieces, heavy, dtype=jnp.bfloat16):
    entries = deviation * jax.random.normal(key, shape, jnp.float32)
    if pieces:
        entries = entries * shard_levels(key, shape, pieces, -0.22, 0.18)
    return jnp.clip(strengthened(entries, jax.random.fold_in(key, 3), *heavy), -limit, limit).astype(dtype)


def setup_inputs(seed: int = 0) -> dict:
    key_list = jax.random.split(jax.random.key(seed), 9)
    train_gate = gaussian_with(key_list[0], (EXPERTS, D_MODEL, D_EXPERT), D_MODEL ** -0.5, 0.1875, ((0, 4), (1, 8)), (1, 2, 8, 2.0), jnp.float32)
    other_gate = bell_draw(key_list[1], (EXPERTS, D_MODEL, D_EXPERT), (D_MODEL * 4) ** -0.5, 0.0625, ((0, 4), (1, 8)))
    train_up = gaussian_with(key_list[2], (EXPERTS, D_MODEL, D_EXPERT), D_MODEL ** -0.5, 0.1875, ((0, 4), (1, 8)), (1, 2, 8, 2.0), jnp.float32)
    other_up = bell_draw(key_list[3], (EXPERTS, D_MODEL, D_EXPERT), (D_MODEL * 4) ** -0.5, 0.0625, ((0, 4), (1, 8)))
    train_down = gaussian_with(key_list[4], (EXPERTS, D_EXPERT, D_MODEL), D_EXPERT ** -0.5, 0.25, ((0, 4), (2, 8)), (2, 1, 8, 2.0), jnp.float32)
    other_down = bell_draw(key_list[5], (EXPERTS, D_EXPERT, D_MODEL), (D_EXPERT * 4) ** -0.5, 0.09375, ((0, 4), (2, 8)))
    router_weight = bell_draw(key_list[6], (D_MODEL, EXPERTS), D_MODEL ** -0.5, 0.125, ((0, 8), (1, 4)), jnp.float32)
    router_gain = jnp.clip(1.0 + 0.15 * jax.random.normal(key_list[7], (D_MODEL,), jnp.float32), 0.25, 1.75)
    return {"train_gate": train_gate, "other_gate": other_gate, "train_up": train_up, "other_up": other_up, "train_down": train_down, "other_down": other_down, "router_weight": router_weight, "router_gain": router_gain}


def reference(train_gate, other_gate, train_up, other_up, train_down, other_down, router_weight, router_gain):
    latest_gate = train_gate + other_gate.astype(jnp.float32)
    latest_up = train_up + other_up.astype(jnp.float32)
    latest_down = train_down + other_down.astype(jnp.float32)
    scale_gate = jnp.max(jnp.abs(latest_gate), axis=1)
    ready_gate = (latest_gate / jnp.expand_dims(scale_gate, 1)).astype(jnp.bfloat16)
    scale_up = jnp.max(jnp.abs(latest_up), axis=1)
    ready_up = (latest_up / jnp.expand_dims(scale_up, 1)).astype(jnp.bfloat16)
    scale_down = jnp.max(jnp.abs(latest_down), axis=2)
    ready_down = (latest_down / jnp.expand_dims(scale_down, 2)).astype(jnp.bfloat16)
    serve_router = (router_weight * router_gain[:, None]).astype(jnp.bfloat16)
    return ready_gate, ready_up, ready_down, scale_gate, scale_up, scale_down, serve_router
```

```python
import functools

import jax
import jax.numpy as jnp
from jax import lax
from jax.experimental import pallas as pl
from jax.experimental.pallas import tpu as pltpu
from jax.sharding import PartitionSpec as P

LANES = 128
MESH = pl.DeviceIdType.MESH


def widest(x):
    most = jnp.abs(x[:, :LANES])
    for at in range(LANES, x.shape[1], LANES):
        most = jnp.maximum(most, jnp.abs(x[:, at : at + LANES]))
    return jnp.max(most.T, axis=0, keepdims=True)


def maxima_kernel(tg, og, tu, ou, td, od, sg, su, sd):
    for train, other, scale in ((tg, og, sg), (tu, ou, su)):
        latest = train[0] + other[0].astype(jnp.float32)
        scale[0] = jnp.max(jnp.abs(latest), axis=0, keepdims=True)
    sd[0] = widest(td[0] + od[0].astype(jnp.float32))


def narrow_kernel(tg, og, tu, ou, td, od, sg, su, sd, ng, nu, nd):
    parts = ng.shape[0]
    for train, other, scale, out in ((tg, og, sg, ng), (tu, ou, su, nu)):
        share = 1.0 / scale[0]
        wide = out.shape[3]
        latest = (train[0] + other[0].astype(jnp.float32)) * share
        latest = latest.astype(jnp.bfloat16)
        for j in range(parts):
            out[j, 0] = latest[:, j * wide : (j + 1) * wide]
    tall = nd.shape[2]
    share = jnp.broadcast_to(1.0 / sd[0], (LANES, sd.shape[2])).T
    for at in range(0, td.shape[2], LANES):
        here = slice(at, at + LANES)
        latest = (td[0, :, here] + od[0, :, here].astype(jnp.float32)) * share
        latest = latest.astype(jnp.bfloat16)
        for j in range(parts):
            nd[j, 0, :, here] = latest[j * tall : (j + 1) * tall]


def exchange_kernel(parts, ng, nu, nd, rg, ru, rd, send_sem, recv_sem, own_sem):
    me = lax.axis_index("rows")
    barrier = pltpu.get_barrier_semaphore()
    for k in range(1, parts):
        pl.semaphore_signal(
            barrier, inc=1, device_id={"rows": lax.rem(me + k, parts)}, device_id_type=MESH
        )
    pl.semaphore_wait(barrier, parts - 1)

    tall, wide = ng.shape[2], nd.shape[3]
    mine = pl.ds(pl.multiple_of(me * tall, tall), tall)
    columns = pl.ds(pl.multiple_of(me * wide, wide), wide)
    places = (
        (ng, rg.at[:, mine, :]),
        (nu, ru.at[:, mine, :]),
        (nd, rd.at[:, :, columns]),
    )
    copies, own = [], []
    for t, (narrow, place) in enumerate(places):
        for k in range(1, parts):
            peer = lax.rem(me + k, parts)
            copy = pltpu.make_async_remote_copy(
                src_ref=narrow.at[peer],
                dst_ref=place,
                send_sem=send_sem.at[t, k - 1],
                recv_sem=recv_sem.at[t, k - 1],
                device_id={"rows": peer},
                device_id_type=MESH,
            )
            copy.start()
            copies.append(copy)
        copy = pltpu.make_async_copy(narrow.at[me], place, own_sem.at[t])
        copy.start()
        own.append(copy)
    for copy in own + copies:
        copy.wait()


def shards(
    parts, train_gate, other_gate, train_up, other_up, train_down, other_down, router_weight, router_gain
):
    weights = (train_gate, other_gate, train_up, other_up, train_down, other_down)
    experts, tall, inner = train_gate.shape
    wide = train_down.shape[2]
    piece = inner // parts
    f32, bf16 = jnp.float32, jnp.bfloat16

    whole = [pl.BlockSpec((1,) + w.shape[1:], lambda e: (e, 0, 0)) for w in weights]
    row = pl.BlockSpec((1, 1, inner), lambda e: (e, 0, 0))
    read = sum(w.size * w.dtype.itemsize for w in weights)
    maxima = pl.pallas_call(
        maxima_kernel,
        grid=(experts,),
        in_specs=whole,
        out_specs=[row] * 3,
        out_shape=[jax.ShapeDtypeStruct((experts, 1, inner), f32)] * 3,
        cost_estimate=pl.CostEstimate(flops=read, bytes_accessed=read, transcendentals=0),
    )(*weights)
    scales = lax.pmax(tuple(maxima), "rows")

    cut = [(parts, experts, tall, piece)] * 2 + [(parts, experts, piece, wide)]
    narrow = pl.pallas_call(
        narrow_kernel,
        grid=(experts,),
        in_specs=whole + [row] * 3,
        out_specs=[pl.BlockSpec((s[0], 1) + s[2:], lambda e: (0, e, 0, 0)) for s in cut],
        out_shape=[jax.ShapeDtypeStruct(s, bf16) for s in cut],
        cost_estimate=pl.CostEstimate(flops=read, bytes_accessed=2 * read, transcendentals=0),
    )(*weights, *scales)

    anywhere = pl.BlockSpec(memory_space=pl.ANY)
    ready_shape = [(experts, parts * tall, piece)] * 2 + [(experts, piece, parts * wide)]
    ready_gate, ready_up, ready_down = pl.pallas_call(
        functools.partial(exchange_kernel, parts),
        in_specs=[anywhere] * 3,
        out_specs=[anywhere] * 3,
        out_shape=[jax.ShapeDtypeStruct(s, bf16) for s in ready_shape],
        scratch_shapes=[
            pltpu.SemaphoreType.DMA((3, parts - 1)),
            pltpu.SemaphoreType.DMA((3, parts - 1)),
            pltpu.SemaphoreType.DMA((3,)),
        ],
        compiler_params=pltpu.CompilerParams(collective_id=0, has_side_effects=True),
    )(*narrow)

    at = lax.axis_index("rows") * piece
    scale_gate, scale_up, scale_down = (
        lax.dynamic_slice_in_dim(s[:, 0, :], at, piece, axis=1) for s in scales
    )
    part_router = (router_weight * router_gain[:, None]).astype(bf16)
    row_router = lax.all_gather(part_router, "rows", axis=0, tiled=True)
    serve_router = lax.all_gather(row_router, "owner", axis=1, tiled=True)
    return (ready_gate, ready_up, ready_down, scale_gate, scale_up, scale_down, serve_router)


def solution(mesh):
    placed = (
        P("owner", "rows", None),
        P("owner", "rows", None),
        P("owner", "rows", None),
        P("owner", "rows", None),
        P("owner", None, "rows"),
        P("owner", None, "rows"),
        P("rows", "owner"),
        P("rows"),
    )
    return jax.shard_map(
        functools.partial(shards, mesh.shape["rows"]),
        mesh=mesh,
        in_specs=placed,
        out_specs=(
            P("owner", None, "rows"),
            P("owner", None, "rows"),
            P("owner", "rows", None),
            P("owner", "rows"),
            P("owner", "rows"),
            P("owner", "rows"),
            P(),
        ),
        check_vma=False,
    )
```
